32 devices in a mesh: leaf: 4 (over y, core), grid: 8 (over z, x).
Axes of the slice: x: 2, y: 2, z: 4, core: 2. Of those that a mesh axis runs over, the one named last changes fastest.
Arguments:
- ainv_sep: bfloat16 [4, 2048, 2048], P('leaf', 'grid'), may hold values from -6 to 6
- l_panel: bfloat16 [4, 2048, 512], P('leaf', 'grid'), may hold values from -0.125 to 0.125
- block_mask: int32 [4, 1, 4], P('leaf'), may hold values 0 or 1
- owner: int32 [4, 4], P('leaf'), may hold values 0 or 1
- dinv: float32 [4, 512, 512], P('leaf', 'grid'), may hold values from -6 to 6
Outputs:
- ainv_panel: bfloat16 [4, 2048, 512], P('leaf', 'grid')
- ainv_upper: bfloat16 [4, 512, 2048], P('leaf', 'grid')
- ainv_diag: float32 [4, 512, 512], P('leaf', 'grid')
The draws below stay inside these ranges and needn't reach their ends.
All inputs are finite; a program needn't handle non-finite values. No bound on the sum of `block_mask` or of `owner` on one device may be relied on, other than what follows from the above.
Results may differ from the reference program's by a relative error of at most 0.0019.
Values may be sent and summed in bfloat16 or wider, within the bound.
No kernel may reach another device: no remote copies, remote signals or barrier semaphores. Data moves between devices by JAX's collectives and lax.ppermute only.
A program may use at most 128 MiB of HBM per device.

```python
import jax
import jax.numpy as jnp
from jax import lax

B = 512
NSUP = 1
SEP = 2048
NB = 4
W = 512
N_LEAF = 4


def with_ends(drawn, key, least, high):
    place = [jax.random.randint(jax.random.fold_in(key, axis), (), 0, length) for axis, length in enumerate(drawn.shape)]
    longest = drawn.shape.index(max(drawn.shape))
    beside = place[:longest] + [(place[longest] + 1) % drawn.shape[longest]] + place[longest + 1:]
    return drawn.at[tuple(place)].set(least).at[tuple(beside)].set(high)


def shard_levels(rng, shape, split, least, largest):
    level, own = 1.0, jax.random.fold_in(rng, 6)
    for position, parts in split:
        draws = jnp.exp(jax.random.uniform(jax.random.fold_in(own, position), (parts,), jnp.float32, least / len(split), largest / len(split)))
        level = level * jnp.repeat(draws, shape[position] // parts).reshape([-1 if axis == position else 1 for axis in range(len(shape))])
    return level


def normal_values(rng, shape, deviation, limit, pieces=(), dtype=jnp.bfloat16):
    array = deviation * jax.random.normal(rng, shape, jnp.float32)
    if pieces:
        array = array * shard_levels(rng, shape, pieces, -0.22, 0.18)
    return jnp.clip(array, -limit, limit).astype(dtype)


def setup_inputs(seed: int = 0) -> dict:
    key_list = jax.random.split(jax.random.key(seed), 6)
    ainv_sep = normal_values(key_list[0], (N_LEAF, SEP, SEP), 1.0, 6.0, ((0, 4), (1, 8)))
    l_panel = normal_values(key_list[1], (N_LEAF, SEP, W), SEP ** -0.5, 0.125, ((0, 4), (1, 8)))
    block_mask = with_ends((jax.random.randint(key_list[2], (N_LEAF, NSUP, NB), 0, 3) < 2).astype(jnp.int32), jax.random.fold_in(key_list[2], 1), 0, 1)
    owner = with_ends((jax.random.randint(key_list[3], (N_LEAF, NB), 0, 2) < 1).astype(jnp.int32), jax.random.fold_in(key_list[3], 1), 0, 1)
    dinv = normal_values(key_list[4], (N_LEAF, W, B), 1.0, 6.0, ((0, 4), (1, 8)), jnp.float32)
    return dict(ainv_sep=ainv_sep, l_panel=l_panel, block_mask=block_mask, owner=owner, dinv=dinv)


def reference(ainv_sep, l_panel, block_mask, owner, dinv):
    panels = []
    uppers = []
    diags = []
    for group in range(N_LEAF):
        own_block = ainv_sep[group].astype(jnp.float32)
        sibling = ainv_sep[group ^ 1].astype(jnp.float32)
        colmask = jnp.repeat(owner[group], B)
        mixed = jnp.where(colmask[None, :] == 1, sibling, own_block)
        rowmask = jnp.repeat(jnp.repeat(block_mask[group].T, B, axis=0), B, axis=1)
        masked = jnp.where(rowmask == 1, l_panel[group], jnp.zeros((), jnp.bfloat16)).astype(jnp.float32)
        panel = (-jnp.dot(mixed, masked, precision=lax.Precision.HIGHEST)).astype(jnp.bfloat16)
        panels.append(panel)
        uppers.append(panel.T)
        panel_f = panel.astype(jnp.float32).reshape(SEP, NSUP, B)
        masked_f = masked.reshape(SEP, NSUP, B)
        update = jnp.einsum("ski,skc->kic", panel_f, masked_f, precision=lax.Precision.HIGHEST)
        diags.append(dinv[group] - update.reshape(NSUP * B, B))
    return jnp.stack(panels), jnp.stack(uppers), jnp.stack(diags)
```

```python
import jax
import jax.numpy as jnp
from jax import lax
from jax.sharding import PartitionSpec as P

B = 512


def swapped(array, axis, stride):
    return lax.ppermute(array, axis, [(i, i ^ 1 << stride) for i in range(lax.axis_size(axis))])


def ring_place(device, size):
    return jnp.where(device % 2 == 0, device // 2, size - 1 - device // 2)


def ring_device(place, size):
    return jnp.where(place < size // 2, 2 * place, 2 * (size - 1 - place) + 1)


def body(ainv_sep, l_panel, block_mask, owner, dinv):
    size = lax.axis_size("grid")
    rows = ainv_sep.shape[1]
    width = l_panel.shape[2]
    half = width // 2
    order = [i for i in range(0, size, 2)] + [i for i in range(size - 1, 0, -2)]
    ahead = [(order[i], order[(i + 1) % size]) for i in range(size)]
    back = [(b, a) for a, b in ahead]
    me = lax.axis_index("grid")
    place = ring_place(me, size)

    own = l_panel[0]
    parts = (own[:, :half], own[:, half:])
    strips = [(me, parts[0], parts[1])]
    f, b = list(parts), list(parts)
    for s in range(1, size // 2):
        f[0] = lax.ppermute(f[0], "grid", ahead)
        b[1] = lax.ppermute(b[1], "grid", back)
        f[1] = lax.ppermute(f[1], "grid", ahead)
        b[0] = lax.ppermute(b[0], "grid", back)
        strips.append((ring_device((place - s) % size, size), f[0], f[1]))
        strips.append((ring_device((place + s) % size, size), b[0], b[1]))
    last0 = lax.ppermute(f[0], "grid", ahead)
    last1 = lax.ppermute(b[1], "grid", back)
    strips.append((ring_device((place + size // 2) % size, size), last0, last1))

    sibling = swapped(ainv_sep, "leaf", 0)
    col_owner = jnp.repeat(owner[0], B)
    col_flag = jnp.repeat(block_mask[0, 0], B)
    mixed = jnp.where(col_owner[None, :] == 1, sibling[0], ainv_sep[0])
    mixed = jnp.where(col_flag[None, :] == 1, mixed, jnp.zeros((), jnp.bfloat16))

    sums = [jnp.zeros((rows, half), jnp.float32) for _ in range(2)]
    for source, left, right in strips:
        columns = lax.dynamic_slice_in_dim(mixed, source * rows, rows, 1)
        sums[0] = sums[0] + jnp.dot(columns, left, preferred_element_type=jnp.float32)
        sums[1] = sums[1] + jnp.dot(columns, right, preferred_element_type=jnp.float32)
    panel = jnp.concatenate([(-s).astype(jnp.bfloat16) for s in sums], axis=1)
    upper = lax.all_to_all(panel.T, "grid", split_axis=0, concat_axis=1, tiled=True)
    kept = jnp.where(col_flag[None, :] == 1, upper, jnp.zeros((), jnp.bfloat16))
    updates = [jnp.zeros((upper.shape[0], half), jnp.float32) for _ in range(2)]
    for source, left, right in strips:
        columns = lax.dynamic_slice_in_dim(kept, source * rows, rows, 1)
        updates[0] = updates[0] + jnp.dot(columns, left, preferred_element_type=jnp.float32)
        updates[1] = updates[1] + jnp.dot(columns, right, preferred_element_type=jnp.float32)
    diag = dinv[0] - jnp.concatenate(updates, axis=1)
    return (panel[None], upper[None], diag[None])


def solution(mesh):
    placed = (
        P("leaf", "grid", None),
        P("leaf", "grid", None),
        P("leaf", None, None),
        P("leaf", None),
        P("leaf", "grid", None),
    )
    return jax.shard_map(
        body,
        mesh=mesh,
        in_specs=placed,
        out_specs=(P("leaf", "grid", None), P("leaf", "grid", None), P("leaf", "grid", None)),
        check_vma=False,
    )
```

```python
import jax
import jax.numpy as jnp
from jax import lax
from jax.sharding import PartitionSpec as P

B = 512


def swapped(array, axis, stride):
    return lax.ppermute(array, axis, [(i, i ^ 1 << stride) for i in range(lax.axis_size(axis))])


def ring_place(device, size):
    return jnp.where(device % 2 == 0, device // 2, size - 1 - device // 2)


def ring_device(place, size):
    return jnp.where(place < size // 2, 2 * place, 2 * (size - 1 - place) + 1)


def body(ainv_sep, l_panel, block_mask, owner, dinv):
    size = lax.axis_size("grid")
    rows = ainv_sep.shape[1]
    width = l_panel.shape[2]
    half = width // 2
    order = [i for i in range(0, size, 2)] + [i for i in range(size - 1, 0, -2)]
    ahead = [(order[i], order[(i + 1) % size]) for i in range(size)]
    back = [(b, a) for a, b in ahead]
    me = lax.axis_index("grid")
    place = ring_place(me, size)

    own = l_panel[0]
    parts = (own[:, :half], own[:, half:])
    strips = [(me, parts[0], parts[1])]
    f, b = list(parts), list(parts)
    for s in range(1, size // 2):
        f[0] = lax.ppermute(f[0], "grid", ahead)
        b[1] = lax.ppermute(b[1], "grid", back)
        f[1] = lax.ppermute(f[1], "grid", ahead)
        b[0] = lax.ppermute(b[0], "grid", back)
        strips.append((ring_device((place - s) % size, size), f[0], f[1]))
        strips.append((ring_device((place + s) % size, size), b[0], b[1]))
    sibling = swapped(ainv_sep, "leaf", 0)
    col_owner = jnp.repeat(owner[0], B)
    col_flag = jnp.repeat(block_mask[0, 0], B)
    mixed = jnp.where(col_owner[None, :] == 1, sibling[0], ainv_sep[0])
    mixed = jnp.where(col_flag[None, :] == 1, mixed, jnp.zeros((), jnp.bfloat16))

    def added(sums, group):
        for source, left, right in group:
            columns = lax.dynamic_slice_in_dim(mixed, source * rows, rows, 1)
            sums = [
                sums[0] + jnp.dot(columns, left, preferred_element_type=jnp.float32),
                sums[1] + jnp.dot(columns, right, preferred_element_type=jnp.float32),
            ]
        return sums

    early = 1
    sums = added([jnp.zeros((rows, half), jnp.float32) for _ in range(2)], strips[:early])
    sums[0], sums[1], f[0], b[1] = lax.optimization_barrier((sums[0], sums[1], f[0], b[1]))
    last0 = lax.ppermute(f[0], "grid", ahead)
    last1 = lax.ppermute(b[1], "grid", back)
    strips.append((ring_device((place + size // 2) % size, size), last0, last1))
    sums = added(sums, strips[early:])
    panel = jnp.concatenate([(-s).astype(jnp.bfloat16) for s in sums], axis=1)
    upper = lax.all_to_all(panel.T, "grid", split_axis=0, concat_axis=1, tiled=True)
    kept = jnp.where(col_flag[None, :] == 1, upper, jnp.zeros((), jnp.bfloat16))
    updates = [jnp.zeros((upper.shape[0], half), jnp.float32) for _ in range(2)]
    for source, left, right in strips:
        columns = lax.dynamic_slice_in_dim(kept, source * rows, rows, 1)
        updates[0] = updates[0] + jnp.dot(columns, left, preferred_element_type=jnp.float32)
        updates[1] = updates[1] + jnp.dot(columns, right, preferred_element_type=jnp.float32)
    diag = dinv[0] - jnp.concatenate(updates, axis=1)
    return (panel[None], upper[None], diag[None])


def solution(mesh):
    placed = (
        P("leaf", "grid", None),
        P("leaf", "grid", None),
        P("leaf", None, None),
        P("leaf", None),
        P("leaf", "grid", None),
    )
    return jax.shard_map(
        body,
        mesh=mesh,
        in_specs=placed,
        out_specs=(P("leaf", "grid", None), P("leaf", "grid", None), P("leaf", "grid", None)),
        check_vma=False,
    )
```

```python
import jax
import jax.numpy as jnp
from jax import lax
from jax.sharding import PartitionSpec as P

B = 512


def swapped(array, axis, stride):
    return lax.ppermute(array, axis, [(i, i ^ 1 << stride) for i in range(lax.axis_size(axis))])


def ring_place(device, size):
    return jnp.where(device % 2 == 0, device // 2, size - 1 - device // 2)


def ring_device(place, size):
    return jnp.where(place < size // 2, 2 * place, 2 * (size - 1 - place) + 1)


def body(ainv_sep, l_panel, block_mask, owner, dinv):
    size = lax.axis_size("grid")
    rows = ainv_sep.shape[1]
    width = l_panel.shape[2]
    half = width // 2
    order = [i for i in range(0, size, 2)] + [i for i in range(size - 1, 0, -2)]
    ahead = [(order[i], order[(i + 1) % size]) for i in range(size)]
    back = [(b, a) for a, b in ahead]
    me = lax.axis_index("grid")
    place = ring_place(me, size)

    own = l_panel[0]
    parts = (own[:, :half], own[:, half:])
    strips = [(me, parts[0], parts[1])]
    f, b = list(parts), list(parts)
    for s in range(1, size // 2):
        f[0] = lax.ppermute(f[0], "grid", ahead)
        b[1] = lax.ppermute(b[1], "grid", back)
        f[1] = lax.ppermute(f[1], "grid", ahead)
        b[0] = lax.ppermute(b[0], "grid", back)
        strips.append((ring_device((place - s) % size, size), f[0], f[1]))
        strips.append((ring_device((place + s) % size, size), b[0], b[1]))
    ainv_sep, f[0] = lax.optimization_barrier((ainv_sep, f[0]))
    sibling = swapped(ainv_sep, "leaf", 0)
    col_owner = jnp.repeat(owner[0], B)
    col_flag = jnp.repeat(block_mask[0, 0], B)
    mixed = jnp.where(col_owner[None, :] == 1, sibling[0], ainv_sep[0])
    mixed = jnp.where(col_flag[None, :] == 1, mixed, jnp.zeros((), jnp.bfloat16))

    def added(sums, group):
        for source, left, right in group:
            columns = lax.dynamic_slice_in_dim(mixed, source * rows, rows, 1)
            sums = [
                sums[0] + jnp.dot(columns, left, preferred_element_type=jnp.float32),
                sums[1] + jnp.dot(columns, right, preferred_element_type=jnp.float32),
            ]
        return sums

    early = 1
    sums = added([jnp.zeros((rows, half), jnp.float32) for _ in range(2)], strips[:early])
    sums[0], sums[1], f[0], b[1] = lax.optimization_barrier((sums[0], sums[1], f[0], b[1]))
    last0 = lax.ppermute(f[0], "grid", ahead)
    last1 = lax.ppermute(b[1], "grid", back)
    strips.append((ring_device((place + size // 2) % size, size), last0, last1))
    sums = added(sums, strips[early:])
    panel = jnp.concatenate([(-s).astype(jnp.bfloat16) for s in sums], axis=1)
    upper = lax.all_to_all(panel.T, "grid", split_axis=0, concat_axis=1, tiled=True)
    kept = jnp.where(col_flag[None, :] == 1, upper, jnp.zeros((), jnp.bfloat16))
    updates = [jnp.zeros((upper.shape[0], half), jnp.float32) for _ in range(2)]
    for source, left, right in strips:
        columns = lax.dynamic_slice_in_dim(kept, source * rows, rows, 1)
        updates[0] = updates[0] + jnp.dot(columns, left, preferred_element_type=jnp.float32)
        updates[1] = updates[1] + jnp.dot(columns, right, preferred_element_type=jnp.float32)
    diag = dinv[0] - jnp.concatenate(updates, axis=1)
    return (panel[None], upper[None], diag[None])


def solution(mesh):
    placed = (
        P("leaf", "grid", None),
        P("leaf", "grid", None),
        P("leaf", None, None),
        P("leaf", None),
        P("leaf", "grid", None),
    )
    return jax.shard_map(
        body,
        mesh=mesh,
        in_specs=placed,
        out_specs=(P("leaf", "grid", None), P("leaf", "grid", None), P("leaf", "grid", None)),
        check_vma=False,
    )
```
